32 devices in a mesh: ctx: 8 (over z, y), mp: 4 (over x, core).
Axes of the slice: x: 2, y: 2, z: 4, core: 2. Of those that a mesh axis runs over, the one named last changes fastest.
Arguments:
- queries: bfloat16 [2048, 4096], P('ctx', 'mp'), may hold values from -20 to 20
- keys: bfloat16 [2048, 2048], P('ctx', 'mp'), may hold values from -20 to 20
- values: bfloat16 [2048, 2048], P('ctx', 'mp'), may hold values from -6 to 6
- out_grad: bfloat16 [2048, 4608], P('ctx', 'mp'), may hold values from -6 to 6
- doc_ids: int32 [2048], P('ctx'), may hold values from 0 to 7, never falling along the last dimension, each value on 1 to 768 neighbouring positions
- w_out: bfloat16 [4096, 4608], P('mp'), may hold values from -0.09375 to 0.09375
Outputs:
- query_gradient: bfloat16 [2048, 4096], P('ctx', 'mp')
- key_gradient: bfloat16 [2048, 2048], P('ctx', 'mp')
- value_gradient: bfloat16 [2048, 2048], P('ctx', 'mp')
The draws below stay inside these ranges and needn't reach their ends.
Inputs may be any that keep to these rules, and one draw needn't show every extreme that they name: `doc_ids`: document numbers never fall along the sequence; every document has at most (3) * 256 tokens, and some document has exactly that many.
All inputs are finite; a program needn't handle non-finite values.
Results may differ from the reference program's by a relative error of at most 0.0069.
Values may be sent and summed in bfloat16 or wider, within the bound.
A program may use at most 64 MiB of HBM per device.

```python
import math
import jax
import jax.numpy as jnp
import numpy as np
from jax import lax

D = 4608
QUERY_HEADS = 32
KEY_VALUE_HEADS = 16
HEAD_SIZE = 128
SHARD_TOKENS = 256
SPAN = 4
PACKED_TOKENS = 2048
N_CTX = 8


def shared_parts(key):
    joint_factor = jax.random.fold_in(key, 7100)
    selected_rows = jax.random.randint(jax.random.fold_in(joint_factor, 1), (PACKED_TOKENS, KEY_VALUE_HEADS), 0, 32) == 0
    travel_sense = jax.random.normal(jax.random.fold_in(joint_factor, 2), (KEY_VALUE_HEADS, HEAD_SIZE), jnp.float32)
    travel_sense = travel_sense / jnp.sqrt(jnp.sum(travel_sense * travel_sense, axis=1, keepdims=True))
    return (selected_rows, travel_sense)


def seed_jitter(key, shape):
    return jnp.clip(jax.random.normal(key, shape, jnp.float32), -6.0, 6.0)


def magnitude(key, shape):
    return jnp.exp(jax.random.uniform(key, shape, jnp.float32, jnp.log(17.3), jnp.log(30.0)))


def draw_queries(key, part):
    query_groups = QUERY_HEADS // KEY_VALUE_HEADS
    selected_rows, travel_sense = shared_parts(key)
    local_portion = jax.random.fold_in(key, 7201)
    jitter = seed_jitter(jax.random.fold_in(local_portion, 1), (PACKED_TOKENS, KEY_VALUE_HEADS, query_groups, HEAD_SIZE))
    multiplier = magnitude(jax.random.fold_in(local_portion, 2), (PACKED_TOKENS, KEY_VALUE_HEADS, query_groups))
    multiplier = jnp.where(selected_rows[:, :, None], multiplier, 0.0)
    final_output = jitter + multiplier[..., None] * travel_sense[None, :, None, :]
    return jnp.clip(final_output, -20.0, 20.0).reshape(PACKED_TOKENS, QUERY_HEADS * HEAD_SIZE).astype(jnp.bfloat16)


def draw_keys(key, part):
    selected_rows, travel_sense = shared_parts(key)
    local_portion = jax.random.fold_in(key, 7302)
    jitter = seed_jitter(jax.random.fold_in(local_portion, 1), (PACKED_TOKENS, KEY_VALUE_HEADS, HEAD_SIZE))
    multiplier = magnitude(jax.random.fold_in(local_portion, 2), (PACKED_TOKENS, KEY_VALUE_HEADS))
    multiplier = jnp.where(selected_rows, multiplier, 0.0)
    final_output = jitter + multiplier[..., None] * travel_sense[None, :, :]
    return jnp.clip(final_output, -20.0, 20.0).reshape(PACKED_TOKENS, KEY_VALUE_HEADS * HEAD_SIZE).astype(jnp.bfloat16)


def block_levels(stream_key, extent, split, least, largest):
    def one(dim, blocks):
        heights = jax.random.uniform(jax.random.fold_in(jax.random.fold_in(stream_key, 6), dim), (blocks,), jnp.float32, least / len(split), largest / len(split))
        return jnp.repeat(jnp.exp(heights), extent[dim] // blocks).reshape((-1,) + (1,) * (len(extent) - dim - 1))

    loudness = one(*split[0])
    for cut in split[1:]:
        loudness = loudness * one(*cut)
    return loudness


def profile(amount, total, reach, slope):
    loads = [(1 << 20) // math.isqrt(rank ** slope) + 1 for rank in range(2, amount + 1)]
    spare, given = total - reach - (amount - 1), [1] * (amount - 1)
    while spare > 0:
        candidates = [i for i in range(amount - 1) if given[i] < reach]
        pool, remaining = sum([loads[i] for i in candidates]), spare
        for i in candidates:
            addition = min(reach - given[i], max(1, remaining * loads[i] // pool), spare)
            given[i] = given[i] + addition
            spare = spare - addition
    return np.array([reach] + given)


def uneven_parts(own_key, amount, total, bound, lean):
    if amount == 2:
        one = jax.random.randint(own_key, (), max(1, total - bound), min(bound, total - 1) + 1)
        return jnp.stack([one, total - one])
    tallies = jnp.asarray(profile(amount, total, bound, lean), jnp.int32)
    pairs = (amount - 1) // 2
    source_of, sink = tallies[1:1 + 2 * pairs:2], tallies[2:2 + 2 * pairs:2]
    room = jnp.minimum(source_of - 1, bound - sink)
    shifted = jax.random.randint(jax.random.fold_in(own_key, 1), (pairs,), 0, 1 << 20) % (room + 1)
    tallies = tallies.at[1:1 + 2 * pairs:2].set(source_of - shifted).at[2:2 + 2 * pairs:2].set(sink + shifted)
    return tallies[jax.random.permutation(jax.random.fold_in(own_key, 2), amount)]


def gaussian(key, extent, scale, limit, cuts=(), kind=jnp.bfloat16):
    loudness = block_levels(key, extent, cuts, -0.22, 0.18) if cuts else 1.0
    entries = jax.random.normal(key, extent, jnp.float32) * scale * loudness
    return jnp.minimum(jnp.maximum(entries, -limit), limit).astype(kind)


def setup_inputs(seed: int = 0) -> dict:
    key_of = jax.random.split(jax.random.key(seed), 7)
    queries = draw_queries(jax.random.fold_in(key_of[6], 71), 0)
    keys = draw_keys(jax.random.fold_in(key_of[6], 71), 0)
    values = gaussian(key_of[2], (PACKED_TOKENS, KEY_VALUE_HEADS * HEAD_SIZE), 1.0, 6.0, ((0, 8), (1, 4)))
    out_grad = gaussian(key_of[3], (PACKED_TOKENS, D), 1.0, 6.0, ((0, 8), (1, 4)))
    doc_ids = jnp.searchsorted(jnp.cumsum(uneven_parts(key_of[4], N_CTX, PACKED_TOKENS, (SPAN - 1) * SHARD_TOKENS, 2)), jnp.arange(PACKED_TOKENS), side="right").astype(jnp.int32)
    w_out = gaussian(key_of[5], (QUERY_HEADS * HEAD_SIZE, D), D ** -0.5, 0.09375, ((0, 4),))
    return {"queries": queries, "keys": keys, "values": values, "out_grad": out_grad, "doc_ids": doc_ids, "w_out": w_out}


cap_value = 50.0
query_scale = 1.0 / 12.0


def tile_scores(query_quad, key_slab):
    raw = jnp.einsum("qhgd,khd->hgqk", query_quad.astype(jnp.float32), key_slab.astype(jnp.float32))
    tanh_part = jnp.tanh(raw * (query_scale / cap_value))
    return cap_value * tanh_part, tanh_part


def reference(queries, keys, values, out_grad, doc_ids, w_out):
    query_groups = QUERY_HEADS // KEY_VALUE_HEADS
    visible_span = SPAN * SHARD_TOKENS
    leading_edge = (SPAN - 1) * SHARD_TOKENS
    padded_keys = jnp.concatenate([jnp.zeros((leading_edge, KEY_VALUE_HEADS * HEAD_SIZE), jnp.bfloat16), keys])
    padded_values = jnp.concatenate([jnp.zeros((leading_edge, KEY_VALUE_HEADS * HEAD_SIZE), jnp.bfloat16), values])
    ids_front = jnp.concatenate([jnp.full((leading_edge,), -1, jnp.int32), doc_ids])
    offsets = jnp.arange(SHARD_TOKENS, dtype=jnp.int32)
    spots = jnp.arange(visible_span, dtype=jnp.int32)
    weight_full = w_out.astype(jnp.float32)

    def query_block(index):
        span_opening = (index * SHARD_TOKENS).astype(jnp.int32)
        query_quad = lax.dynamic_slice_in_dim(queries, span_opening, SHARD_TOKENS, 0).reshape(SHARD_TOKENS, KEY_VALUE_HEADS, query_groups, HEAD_SIZE)
        grad_rows = lax.dynamic_slice_in_dim(out_grad, span_opening, SHARD_TOKENS, 0).astype(jnp.float32)
        incoming_gradient = lax.dot_general(grad_rows, weight_full, (((1,), (1,)), ((), ()))).astype(jnp.bfloat16)
        gradient_quad = incoming_gradient.reshape(SHARD_TOKENS, KEY_VALUE_HEADS, query_groups, HEAD_SIZE)
        key_slab = lax.dynamic_slice_in_dim(padded_keys, span_opening, visible_span, 0).reshape(visible_span, KEY_VALUE_HEADS, HEAD_SIZE)
        value_slab = lax.dynamic_slice_in_dim(padded_values, span_opening, visible_span, 0).reshape(visible_span, KEY_VALUE_HEADS, HEAD_SIZE)
        key_ids = lax.dynamic_slice_in_dim(ids_front, span_opening, visible_span, 0)
        query_ids = lax.dynamic_slice_in_dim(doc_ids, span_opening, SHARD_TOKENS, 0)
        key_pos = span_opening - leading_edge + spots
        query_pos = span_opening + offsets
        mask = (query_ids[:, None] == key_ids[None, :]) & (key_pos[None, :] <= query_pos[:, None])
        scores, tanh_part = tile_scores(query_quad, key_slab)
        weights = jnp.where(mask, jnp.exp(scores), 0.0)
        total = jnp.sum(weights, axis=3)
        logsum_total = jnp.log(total)
        value_sum = jnp.einsum("hgqk,khd->qhgd", weights.astype(jnp.bfloat16).astype(jnp.float32), value_slab.astype(jnp.float32))
        attended = value_sum / jnp.transpose(total, (2, 0, 1))[..., None]
        row_correction = jnp.transpose(jnp.sum(gradient_quad.astype(jnp.float32) * attended, axis=3), (1, 2, 0))
        probs = jnp.where(mask, jnp.exp(scores - logsum_total[..., None]), 0.0)
        prob_grad = jnp.einsum("qhgd,khd->hgqk", gradient_quad.astype(jnp.float32), value_slab.astype(jnp.float32))
        logit_grad = (probs * (prob_grad - row_correction[..., None]) * (1.0 - tanh_part * tanh_part) * query_scale).astype(jnp.bfloat16)
        query_part = jnp.einsum("hgqk,khd->qhgd", logit_grad.astype(jnp.float32), key_slab.astype(jnp.float32))
        return (query_part.reshape(SHARD_TOKENS, QUERY_HEADS * HEAD_SIZE).astype(jnp.bfloat16), incoming_gradient,
                jnp.transpose(logsum_total, (2, 0, 1)), jnp.transpose(row_correction, (2, 0, 1)))

    query_gradient, incoming_gradient, logsum_total, row_correction = lax.map(query_block, jnp.arange(N_CTX, dtype=jnp.int32))
    query_gradient = query_gradient.reshape(PACKED_TOKENS, QUERY_HEADS * HEAD_SIZE)
    padded_gradient = jnp.concatenate([incoming_gradient.reshape(PACKED_TOKENS, QUERY_HEADS * HEAD_SIZE), jnp.zeros((leading_edge, QUERY_HEADS * HEAD_SIZE), jnp.bfloat16)])
    padded_queries = jnp.concatenate([queries, jnp.zeros((leading_edge, QUERY_HEADS * HEAD_SIZE), jnp.bfloat16)])
    ids_back = jnp.concatenate([doc_ids, jnp.full((leading_edge,), -1, jnp.int32)])
    padded_logsum = jnp.concatenate([logsum_total.reshape(PACKED_TOKENS, KEY_VALUE_HEADS, query_groups), jnp.zeros((leading_edge, KEY_VALUE_HEADS, query_groups), jnp.float32)])
    padded_correction = jnp.concatenate([row_correction.reshape(PACKED_TOKENS, KEY_VALUE_HEADS, query_groups), jnp.zeros((leading_edge, KEY_VALUE_HEADS, query_groups), jnp.float32)])

    def key_block_grads(index):
        span_opening = (index * SHARD_TOKENS).astype(jnp.int32)
        key_slab = lax.dynamic_slice_in_dim(keys, span_opening, SHARD_TOKENS, 0).reshape(SHARD_TOKENS, KEY_VALUE_HEADS, HEAD_SIZE)
        value_slab = lax.dynamic_slice_in_dim(values, span_opening, SHARD_TOKENS, 0).reshape(SHARD_TOKENS, KEY_VALUE_HEADS, HEAD_SIZE)
        key_ids = lax.dynamic_slice_in_dim(doc_ids, span_opening, SHARD_TOKENS, 0)
        query_quad = lax.dynamic_slice_in_dim(padded_queries, span_opening, visible_span, 0).reshape(visible_span, KEY_VALUE_HEADS, query_groups, HEAD_SIZE)
        gradient_quad = lax.dynamic_slice_in_dim(padded_gradient, span_opening, visible_span, 0).reshape(visible_span, KEY_VALUE_HEADS, query_groups, HEAD_SIZE)
        query_ids = lax.dynamic_slice_in_dim(ids_back, span_opening, visible_span, 0)
        log_rows = jnp.transpose(lax.dynamic_slice_in_dim(padded_logsum, span_opening, visible_span, 0), (1, 2, 0))
        delta_rows = jnp.transpose(lax.dynamic_slice_in_dim(padded_correction, span_opening, visible_span, 0), (1, 2, 0))
        key_pos = span_opening + offsets
        query_pos = span_opening + spots
        mask = (query_ids[:, None] == key_ids[None, :]) & (key_pos[None, :] <= query_pos[:, None])
        scores, tanh_part = tile_scores(query_quad, key_slab)
        probs = jnp.where(mask, jnp.exp(scores - log_rows[..., None]), 0.0)
        prob_grad = jnp.einsum("qhgd,khd->hgqk", gradient_quad.astype(jnp.float32), value_slab.astype(jnp.float32))
        logit_grad = (probs * (prob_grad - delta_rows[..., None]) * (1.0 - tanh_part * tanh_part) * query_scale).astype(jnp.bfloat16)
        key_portion = jnp.einsum("hgqk,qhgd->khd", logit_grad.astype(jnp.float32), query_quad.astype(jnp.float32))
        value_portion = jnp.einsum("hgqk,qhgd->khd", probs.astype(jnp.bfloat16).astype(jnp.float32), gradient_quad.astype(jnp.float32))
        return (key_portion.reshape(SHARD_TOKENS, KEY_VALUE_HEADS * HEAD_SIZE).astype(jnp.bfloat16),
                value_portion.reshape(SHARD_TOKENS, KEY_VALUE_HEADS * HEAD_SIZE).astype(jnp.bfloat16))

    key_gradient, value_gradient = lax.map(key_block_grads, jnp.arange(N_CTX, dtype=jnp.int32))
    return query_gradient, key_gradient.reshape(PACKED_TOKENS, KEY_VALUE_HEADS * HEAD_SIZE), value_gradient.reshape(PACKED_TOKENS, KEY_VALUE_HEADS * HEAD_SIZE)
```

```python
import functools

import jax
import jax.numpy as jnp
from jax import lax
from jax.experimental import pallas as pl
from jax.experimental.pallas import tpu as pltpu
from jax.sharding import PartitionSpec as P

QUERY_HEADS = 32
KEY_VALUE_HEADS = 16
HEAD_SIZE = 128
SPAN = 4
GROUPS = QUERY_HEADS // KEY_VALUE_HEADS
CAP = 50.0
SCALE = 1.0 / 12.0

NN = (((1,), (0,)), ((), ()))
NT = (((1,), (1,)), ((), ()))
TN = (((0,), (0,)), ((), ()))


def dot(a, b, dims):
    return lax.dot_general(a, b, dims, preferred_element_type=jnp.float32)


def kernel(
    n, m, heads, rows, width,
    ids_ref, q_ref, k_ref, v_ref, og_ref, w_ref,
    dq_ref, dk_ref, dv_ref,
    kv, og, wv, qb, hacc, hgt, ids, mask, ubuf, wbuf, acc, tot, grad, back, dqb, fin,
    sem_kv, sem_q, sem_og, sem_w, sem_out,
    ids_s, ids_r, fwd_s, fwd_r, ret_s, ret_r, og_s, og_r,
):
    i = lax.axis_index("ctx")
    me = lax.axis_index("mp")
    odd = lax.rem(i, 2) == 1
    even = lax.rem(i, 2) == 0
    chips = m // 2
    partner = me + 1 - 2 * lax.rem(me, 2)
    d = HEAD_SIZE

    def near(step):
        return {"ctx": lax.rem(i + step + n, n)}

    def load_kv(h, part):
        src = k_ref if part == 0 else v_ref
        return pltpu.make_async_copy(src.at[:, pl.ds(h * d, d)], kv.at[0, h, part], sem_kv.at[h, part])

    def load_q(h, g):
        return pltpu.make_async_copy(
            q_ref.at[:, pl.ds((h * GROUPS + g) * d, d)], qb.at[h, pl.ds(g * rows, rows)], sem_q.at[h, g]
        )

    load_og = pltpu.make_async_copy(og_ref, og.at[me], sem_og)

    def load_w(s):
        if width % 128:
            src = w_ref.at[s]
        else:
            src = w_ref.at[:, pl.ds(s * width, width)]
        return pltpu.make_async_copy(src, wv.at[s], sem_w.at[s])

    load_og.start()
    for h in range(heads):
        for part in range(2):
            load_kv(h, part).start()
    for s in range(m):
        load_w(s).start()
    for h in range(heads):
        for g in range(GROUPS):
            load_q(h, g).start()

    barrier = pltpu.get_barrier_semaphore()
    count = m - 1
    for step in range(1, m):
        pl.semaphore_signal(barrier, inc=1, device_id={"mp": lax.rem(me + step, m)}, device_id_type=pl.DeviceIdType.MESH)
    for step in range(1, SPAN):
        for sign in (1, -1):
            there = (i + step < n) if sign == 1 else (i >= step)

            @pl.when(there)
            def _():
                pl.semaphore_signal(barrier, inc=1, device_id=near(sign * step), device_id_type=pl.DeviceIdType.MESH)

            count = count + there.astype(jnp.int32)
    pl.semaphore_wait(barrier, count)

    def remote(src, dst, send, recv, device):
        return pltpu.make_async_remote_copy(
            src_ref=src, dst_ref=dst, send_sem=send, recv_sem=recv, device_id=device,
            device_id_type=pl.DeviceIdType.MESH,
        )

    def send_ids(hop):
        return remote(ids_ref, ids.at[hop - 1], ids_s.at[hop - 1], ids_r.at[hop - 1], near(hop))

    for hop in range(1, SPAN):

        @pl.when(i + hop < n)
        def _():
            send_ids(hop).start()

    def og_across(step):
        return remote(og.at[me], og.at[me], og_s.at[step - 1], og_r.at[step - 1], {"mp": lax.rem(me + 2 * step, m)})

    def og_from(step):
        s = lax.rem(me - 2 * step + m, m)
        return remote(og.at[s], og.at[s], og_s.at[step - 1], og_r.at[step - 1], {"mp": partner})

    def og_pair(step, slot):
        k = chips - 1 + step
        return remote(og.at[slot], og.at[slot], og_s.at[k], og_r.at[k], {"mp": partner})

    load_og.wait()
    for step in range(1, chips):
        og_across(step).start()
    og_pair(0, me).start()

    def two(h):
        return remote(kv.at[0, h], kv.at[2, h], fwd_s.at[0, h], fwd_r.at[0, h], near(2))

    def pair_even(h):
        return remote(kv.at[0, h], kv.at[1, h], fwd_s.at[1, h], fwd_r.at[1, h], near(1))

    def pair_odd(h):
        return remote(kv.at[2, h], kv.at[1, h], fwd_s.at[1, h], fwd_r.at[1, h], near(-1))

    def three(h):
        return remote(kv.at[1, h], kv.at[3, h], fwd_s.at[2, h], fwd_r.at[2, h], near(2))

    for h in range(heads):
        for part in range(2):
            load_kv(h, part).wait()

        @pl.when(i + 2 < n)
        def _():
            two(h).start()

        @pl.when(even)
        def _():
            pair_even(h).start()

    def product(s, first):
        pltpu.make_async_copy(wv.at[s], wv.at[s], sem_w.at[s]).wait()
        half = 4 * d if (heads * GROUPS) % 4 == 0 else d

        def rows_of(r, c):
            at = pl.ds(pl.multiple_of(r * half, half), half)
            part = dot(wv[s, at, :], og[s], NT)
            if first:
                hacc[at, :] = part
            else:
                hacc[at, :] += part
            return c

        lax.fori_loop(0, heads * GROUPS * d // half, rows_of, 0)

    product(me, True)
    og_pair(0, partner).wait_recv()
    product(partner, False)

    for hop in range(1, SPAN):

        @pl.when(i >= hop)
        def _():
            send_ids(hop).wait_recv()

    hops = jnp.minimum(i, SPAN - 1) + 1
    down = lax.broadcasted_iota(jnp.int32, (rows, rows), 0)
    along = lax.broadcasted_iota(jnp.int32, (rows, rows), 1)
    own_ids = ids_ref[0:1, :].astype(jnp.float32)

    def make_mask(hop, row):
        column = jnp.sum(jnp.where(down == along, row, 0.0), axis=1, keepdims=True)
        seen = (column == own_ids) & (down - hop * rows <= along)
        seen = jnp.where(seen, 1.0, 0.0)
        for g in range(GROUPS):
            mask[hop, :, g * rows:(g + 1) * rows] = seen

    make_mask(0, own_ids)
    for hop in range(1, SPAN):

        @pl.when(i >= hop)
        def _():
            make_mask(hop, ids[hop - 1, 0:1, :].astype(jnp.float32))

    for h in range(heads):

        @pl.when(i >= 2)
        def _():
            two(h).wait_recv()

        @pl.when(odd & (i >= 3))
        def _():
            pair_odd(h).start()

        @pl.when(odd | (i >= 2))
        def _():
            pair_even(h).wait_recv()

        @pl.when((i >= 1) & (i + 2 < n))
        def _():
            three(h).start()

    for step in range(1, chips):
        og_from(step).wait_recv()
        og_pair(step, lax.rem(me - 2 * step + m, m)).start()
    for step in range(1, chips):
        product(lax.rem(me - 2 * step + m, m), False)
    for step in range(1, chips):
        s = lax.rem(partner - 2 * step + m, m)
        og_pair(step, s).wait_recv()
        product(s, False)
    for a in range(heads * GROUPS):
        h, g = divmod(a, GROUPS)
        hgt[h, :, g * rows:(g + 1) * rows] = hacc[a * d:(a + 1) * d, :].astype(jnp.bfloat16)
    for h in range(heads):
        for g in range(GROUPS):
            load_q(h, g).wait()

    def put_dq(h, g):
        return pltpu.make_async_copy(
            dqb.at[h, pl.ds(g * rows, rows)], dq_ref.at[:, pl.ds((h * GROUPS + g) * d, d)], sem_q.at[h, g]
        )

    def compute(h):
        q = qb[h]
        acc[...] = jnp.zeros_like(acc)
        tot[...] = jnp.zeros_like(tot)

        def forward(hop, c):
            s = dot(kv[hop, h, 0], q, NT)
            t = jnp.tanh(s * (SCALE / CAP))
            w = jnp.exp(t * CAP) * mask[hop]
            wb = w.astype(jnp.bfloat16)
            wbuf[hop] = wb
            ubuf[hop] = w * (1.0 - t * t)
            tot[...] += jnp.sum(w, axis=0, keepdims=True)
            acc[...] += dot(kv[hop, h, 1], wb, TN)
            return c

        lax.fori_loop(0, hops, forward, 0)
        inverse = 1.0 / tot[0:1, :]
        hg = hgt[h]
        hg32 = hg.astype(jnp.float32)
        delta = jnp.sum(hg32 * acc[...], axis=0, keepdims=True) * inverse
        scaled = (hg32 * inverse).astype(jnp.bfloat16)
        factor = inverse * SCALE
        acc[...] = jnp.zeros_like(acc)

        def backward(hop, c):
            pg = dot(kv[hop, h, 1], hg, NN)
            ds = (ubuf[hop] * ((pg - delta) * factor)).astype(jnp.bfloat16)
            grad[hop, h, 0] = dot(ds, q, NN).astype(jnp.bfloat16)
            grad[hop, h, 1] = dot(wbuf[hop], scaled, NT).astype(jnp.bfloat16)
            acc[...] += dot(kv[hop, h, 0], ds, TN)
            return c

        lax.fori_loop(0, hops, backward, 0)
        dqb[h] = acc[...].T.astype(jnp.bfloat16)

    def from_three(h):
        return remote(grad.at[3, h], back.at[0, h], ret_s.at[0, h], ret_r.at[0, h], near(-2))

    def from_pair(h, step):
        return remote(grad.at[1, h], back.at[1, h], ret_s.at[1, h], ret_r.at[1, h], near(step))

    def from_two(h):
        return remote(grad.at[2, h], back.at[2, h], ret_s.at[2, h], ret_r.at[2, h], near(-2))

    def gather(hop, stage, h):
        total = grad[hop, h].astype(jnp.float32) + back[stage, h].astype(jnp.float32)
        grad[hop, h] = total.astype(jnp.bfloat16)

    def stage_two(h):
        @pl.when((i >= 1) & (i + 2 < n))
        def _():
            from_three(h).wait_recv()
            gather(1, 0, h)

        @pl.when(odd)
        def _():
            from_pair(h, -1).start()

        @pl.when(even & (i >= 2))
        def _():
            from_pair(h, 1).start()

    def stage_three(h):
        @pl.when(odd & (i >= 3))
        def _():
            from_pair(h, 1).wait_recv()
            gather(2, 1, h)
            from_two(h).start()

    def step(h, c):
        @pl.when(i >= 3)
        def _():
            three(h).wait_recv()

        compute(h)

        @pl.when(i >= 3)
        def _():
            from_three(h).start()

        @pl.when(even & (i >= 2))
        def _():
            from_two(h).start()

        for g in range(GROUPS):
            put_dq(h, g).start()

        @pl.when(h >= 1)
        def _():
            stage_two(h - 1)

        @pl.when(h >= 2)
        def _():
            stage_three(h - 2)

        return c

    lax.fori_loop(0, heads, step, 0)
    stage_two(heads - 1)

    def put(h, part):
        dst = dk_ref if part == 0 else dv_ref
        return pltpu.make_async_copy(fin.at[h, part], dst.at[:, pl.ds(h * d, d)], sem_out.at[h, part])

    def finish(h):
        @pl.when(i + 2 < n)
        def _():
            from_two(h).wait_recv()

        @pl.when(even)
        def _():
            from_pair(h, 1).wait_recv()

        total = grad[0, h].astype(jnp.float32)
        total = total + jnp.where(i + 2 < n, back[2, h].astype(jnp.float32), 0.0)
        total = total + jnp.where(even, back[1, h].astype(jnp.float32), 0.0)
        fin[h] = total.astype(jnp.bfloat16)
        for part in range(2):
            put(h, part).start()

    if heads >= 2:
        stage_three(heads - 2)
    stage_three(heads - 1)


    for h in range(heads):
        finish(h)

    for h in range(heads):
        for g in range(GROUPS):
            put_dq(h, g).wait()
        for part in range(2):
            put(h, part).wait()

        @pl.when(i + 2 < n)
        def _():
            two(h).wait_send()

        @pl.when(even | (i >= 3))
        def _():
            pair_even(h).wait_send()

        @pl.when((i >= 1) & (i + 2 < n))
        def _():
            three(h).wait_send()

        @pl.when(i >= 3)
        def _():
            from_three(h).wait_send()

        @pl.when(odd | (i >= 2))
        def _():
            from_pair(h, 1).wait_send()

        @pl.when(i >= 2)
        def _():
            from_two(h).wait_send()

    for hop in range(1, SPAN):

        @pl.when(i + hop < n)
        def _():
            send_ids(hop).wait_send()

    for stp in range(1, chips):
        og_across(stp).wait_send()
    for stp in range(chips):
        og_pair(stp, me).wait_send()


def body(n, m, queries, keys, values, out_grad, doc_ids, w_out):
    rows = queries.shape[0]
    heads = keys.shape[1] // HEAD_SIZE
    width = out_grad.shape[1]
    d = HEAD_SIZE
    wide = GROUPS * rows
    chips = m // 2
    any_space = pl.BlockSpec(memory_space=pl.ANY)
    bf, f32 = jnp.bfloat16, jnp.float32
    dma = pltpu.SemaphoreType.DMA
    w_rows = w_out.shape[0]
    if width % 128:
        w_out = jnp.transpose(w_out.reshape(w_rows, m, width), (1, 0, 2))
    ids = jnp.broadcast_to(doc_ids[None, :], (8, rows))
    return pl.pallas_call(
        functools.partial(kernel, n, m, heads, rows, width),
        out_shape=(
            jax.ShapeDtypeStruct(queries.shape, bf),
            jax.ShapeDtypeStruct(keys.shape, bf),
            jax.ShapeDtypeStruct(values.shape, bf),
        ),
        in_specs=[pl.BlockSpec(memory_space=pltpu.VMEM)] + [any_space] * 5,
        out_specs=(any_space,) * 3,
        scratch_shapes=[
            pltpu.VMEM((SPAN, heads, 2, rows, d), bf),
            pltpu.VMEM((m, rows, width), bf),
            pltpu.VMEM((m, w_rows, width), bf),
            pltpu.VMEM((heads, wide, d), bf),
            pltpu.VMEM((heads * GROUPS * d, rows), f32),
            pltpu.VMEM((heads, d, wide), bf),
            pltpu.VMEM((SPAN - 1, 8, rows), jnp.int32),
            pltpu.VMEM((SPAN, rows, wide), f32),
            pltpu.VMEM((SPAN, rows, wide), f32),
            pltpu.VMEM((SPAN, rows, wide), bf),
            pltpu.VMEM((d, wide), f32),
            pltpu.VMEM((1, wide), f32),
            pltpu.VMEM((SPAN, heads, 2, rows, d), bf),
            pltpu.VMEM((3, heads, 2, rows, d), bf),
            pltpu.VMEM((heads, wide, d), bf),
            pltpu.VMEM((heads, 2, rows, d), bf),
            dma((heads, 2)),
            dma((heads, GROUPS)),
            dma,
            dma((m,)),
            dma((heads, 2)),
            dma((SPAN - 1,)),
            dma((SPAN - 1,)),
            dma((3, heads)),
            dma((3, heads)),
            dma((3, heads)),
            dma((3, heads)),
            dma((2 * chips - 1,)),
            dma((2 * chips - 1,)),
        ],
        compiler_params=pltpu.CompilerParams(
            collective_id=0, has_side_effects=True, vmem_limit_bytes=60 * 1024 * 1024
        ),
    )(ids, queries, keys, values, out_grad, w_out)


def solution(mesh):
    placed = (
        P("ctx", "mp"),
        P("ctx", "mp"),
        P("ctx", "mp"),
        P("ctx", "mp"),
        P("ctx"),
        P("mp", None),
    )
    return jax.shard_map(
        functools.partial(body, mesh.shape["ctx"], mesh.shape["mp"]),
        mesh=mesh,
        in_specs=placed,
        out_specs=(P("ctx", "mp"), P("ctx", "mp"), P("ctx", "mp")),
        check_vma=False,
    )
```

```python
import functools

import jax
import jax.numpy as jnp
from jax import lax
from jax.experimental import pallas as pl
from jax.experimental.pallas import tpu as pltpu
from jax.sharding import PartitionSpec as P

QUERY_HEADS = 32
KEY_VALUE_HEADS = 16
HEAD_SIZE = 128
SPAN = 4
GROUPS = QUERY_HEADS // KEY_VALUE_HEADS
CAP = 50.0
SCALE = 1.0 / 12.0

NN = (((1,), (0,)), ((), ()))
NT = (((1,), (1,)), ((), ()))
TN = (((0,), (0,)), ((), ()))


def dot(a, b, dims):
    return lax.dot_general(a, b, dims, preferred_element_type=jnp.float32)


def kernel(
    n, m, heads, rows, width,
    ids_ref, q_ref, k_ref, v_ref, og_ref, w_ref,
    dq_ref, dk_ref, dv_ref,
    kv, og, wv, qb, hacc, hgt, ids, mask, ubuf, wbuf, acc, tot, grad, back, dqb, fin,
    sem_kv, sem_q, sem_og, sem_w, sem_out,
    ids_s, ids_r, fwd_s, fwd_r, ret_s, ret_r, og_s, og_r,
):
    i = lax.axis_index("ctx")
    me = lax.axis_index("mp")
    odd = lax.rem(i, 2) == 1
    even = lax.rem(i, 2) == 0
    chips = m // 2
    partner = me + 1 - 2 * lax.rem(me, 2)
    d = HEAD_SIZE

    def near(step):
        return {"ctx": lax.rem(i + step + n, n)}

    def load_kv(h, part):
        src = k_ref if part == 0 else v_ref
        return pltpu.make_async_copy(src.at[:, pl.ds(h * d, d)], kv.at[0, h, part], sem_kv.at[h, part])

    def load_q(h, g):
        return pltpu.make_async_copy(
            q_ref.at[:, pl.ds((h * GROUPS + g) * d, d)], qb.at[h, pl.ds(g * rows, rows)], sem_q.at[h, g]
        )

    load_og = pltpu.make_async_copy(og_ref, og.at[me], sem_og)

    def load_w(s):
        if width % 128:
            src = w_ref.at[s]
        else:
            src = w_ref.at[:, pl.ds(s * width, width)]
        return pltpu.make_async_copy(src, wv.at[s], sem_w.at[s])

    load_og.start()
    for h in range(heads):
        for part in range(2):
            load_kv(h, part).start()
    for s in range(m):
        load_w(s).start()
    for h in range(heads):
        for g in range(GROUPS):
            load_q(h, g).start()

    barrier = pltpu.get_barrier_semaphore()
    count = m - 1
    for step in range(1, m):
        pl.semaphore_signal(barrier, inc=1, device_id={"mp": lax.rem(me + step, m)}, device_id_type=pl.DeviceIdType.MESH)
    for step in range(1, SPAN):
        for sign in (1, -1):
            there = (i + step < n) if sign == 1 else (i >= step)

            @pl.when(there)
            def _():
                pl.semaphore_signal(barrier, inc=1, device_id=near(sign * step), device_id_type=pl.DeviceIdType.MESH)

            count = count + there.astype(jnp.int32)
    pl.semaphore_wait(barrier, count)

    def remote(src, dst, send, recv, device):
        return pltpu.make_async_remote_copy(
            src_ref=src, dst_ref=dst, send_sem=send, recv_sem=recv, device_id=device,
            device_id_type=pl.DeviceIdType.MESH,
        )

    def send_ids(hop):
        return remote(ids_ref, ids[hop - 1], ids_s.at[hop - 1], ids_r.at[hop - 1], near(hop))

    for hop in range(1, SPAN):

        @pl.when(i + hop < n)
        def _():
            send_ids(hop).start()

    def og_across(step):
        return remote(og.at[me], og.at[me], og_s.at[step - 1], og_r.at[step - 1], {"mp": lax.rem(me + 2 * step, m)})

    def og_from(step):
        s = lax.rem(me - 2 * step + m, m)
        return remote(og.at[s], og.at[s], og_s.at[step - 1], og_r.at[step - 1], {"mp": partner})

    def og_pair(step, slot):
        k = chips - 1 + step
        return remote(og.at[slot], og.at[slot], og_s.at[k], og_r.at[k], {"mp": partner})

    load_og.wait()
    for step in range(1, chips):
        og_across(step).start()
    og_pair(0, me).start()

    def two(h):
        return remote(kv.at[0, h], kv.at[2, h], fwd_s.at[0, h], fwd_r.at[0, h], near(2))

    def pair_even(h):
        return remote(kv.at[0, h], kv.at[1, h], fwd_s.at[1, h], fwd_r.at[1, h], near(1))

    def pair_odd(h):
        return remote(kv.at[2, h], kv.at[1, h], fwd_s.at[1, h], fwd_r.at[1, h], near(-1))

    def three(h):
        return remote(kv.at[1, h], kv.at[3, h], fwd_s.at[2, h], fwd_r.at[2, h], near(2))

    early = max(heads - 1, 1)

    def send_two(h):
        @pl.when(i + 2 < n)
        def _():
            two(h).start()

    for h in range(heads):
        for part in range(2):
            load_kv(h, part).wait()

        if h < early:
            send_two(h)

        @pl.when(even)
        def _():
            pair_even(h).start()

    def product(s, first):
        pltpu.make_async_copy(wv.at[s], wv.at[s], sem_w.at[s]).wait()
        half = 4 * d if (heads * GROUPS) % 4 == 0 else d

        def rows_of(r, c):
            at = pl.ds(pl.multiple_of(r * half, half), half)
            part = dot(wv[s, at, :], og[s], NT)
            if first:
                hacc[at, :] = part
            else:
                hacc[at, :] += part
            return c

        lax.fori_loop(0, heads * GROUPS * d // half, rows_of, 0)

    product(me, True)
    og_pair(0, partner).wait_recv()
    product(partner, False)

    for hop in range(1, SPAN):

        @pl.when(i >= hop)
        def _():
            send_ids(hop).wait_recv()

    hops = jnp.minimum(i, SPAN - 1) + 1
    down = lax.broadcasted_iota(jnp.int32, (rows, rows), 0)
    along = lax.broadcasted_iota(jnp.int32, (rows, rows), 1)
    own_ids = ids_ref[...].reshape(1, rows).astype(jnp.float32)

    def make_mask(hop, row):
        column = jnp.sum(jnp.where(down == along, row, 0.0), axis=1, keepdims=True)
        seen = (column == own_ids) & (down - hop * rows <= along)
        seen = jnp.where(seen, 1.0, 0.0)
        for g in range(GROUPS):
            mask[hop, :, g * rows:(g + 1) * rows] = seen

    make_mask(0, own_ids)
    for hop in range(1, SPAN):

        @pl.when(i >= hop)
        def _():
            make_mask(hop, ids[hop - 1][...].reshape(1, rows).astype(jnp.float32))

    def relay(h):
        @pl.when(i >= 2)
        def _():
            two(h).wait_recv()

        @pl.when(odd & (i >= 3))
        def _():
            pair_odd(h).start()

        @pl.when(odd | (i >= 2))
        def _():
            pair_even(h).wait_recv()

        @pl.when((i >= 1) & (i + 2 < n))
        def _():
            three(h).start()

        if h == 0:
            for later in range(early, heads):
                send_two(later)

    def put_dq(h, g):
        return pltpu.make_async_copy(
            dqb.at[h, pl.ds(g * rows, rows)], dq_ref.at[:, pl.ds((h * GROUPS + g) * d, d)], sem_q.at[h, g]
        )

    def forward_pass(h):
        @pl.when(i >= 3)
        def _():
            three(h).wait_recv()

        q = qb[h]
        acc[...] = jnp.zeros_like(acc)
        tot[...] = jnp.zeros_like(tot)

        def forward(hop, c):
            s = dot(kv[hop, h, 0], q, NT)
            t = jnp.tanh(s * (SCALE / CAP))
            w = jnp.exp(t * CAP) * mask[hop]
            wb = w.astype(jnp.bfloat16)
            wbuf[hop] = wb
            ubuf[hop] = w * (1.0 - t * t)
            tot[...] += jnp.sum(w, axis=0, keepdims=True)
            acc[...] += dot(kv[hop, h, 1], wb, TN)
            return c

        lax.fori_loop(0, hops, forward, 0)

    def backward_pass(h):
        q = qb[h]
        inverse = 1.0 / tot[0:1, :]
        hg = hgt[h]
        hg32 = hg.astype(jnp.float32)
        delta = jnp.sum(hg32 * acc[...], axis=0, keepdims=True) * inverse
        scaled = (hg32 * inverse).astype(jnp.bfloat16)
        factor = inverse * SCALE
        acc[...] = jnp.zeros_like(acc)

        def backward(hop, c):
            pg = dot(kv[hop, h, 1], hg, NN)
            ds = (ubuf[hop] * ((pg - delta) * factor)).astype(jnp.bfloat16)
            grad[hop, h, 0] = dot(ds, q, NN).astype(jnp.bfloat16)
            grad[hop, h, 1] = dot(wbuf[hop], scaled, NT).astype(jnp.bfloat16)
            acc[...] += dot(kv[hop, h, 0], ds, TN)
            return c

        lax.fori_loop(0, hops, backward, 0)
        dqb[h] = acc[...].T.astype(jnp.bfloat16)
        for g in range(GROUPS):
            put_dq(h, g).start()

    def from_three(h):
        return remote(grad.at[3, h], back.at[0, h], ret_s.at[0, h], ret_r.at[0, h], near(-2))

    def from_pair(h, step):
        return remote(grad.at[1, h], back.at[1, h], ret_s.at[1, h], ret_r.at[1, h], near(step))

    def from_two(h):
        return remote(grad.at[2, h], back.at[2, h], ret_s.at[2, h], ret_r.at[2, h], near(-2))

    def gather(hop, stage, h):
        total = grad[hop, h].astype(jnp.float32) + back[stage, h].astype(jnp.float32)
        grad[hop, h] = total.astype(jnp.bfloat16)

    def stage_two(h):
        @pl.when((i >= 1) & (i + 2 < n))
        def _():
            from_three(h).wait_recv()
            gather(1, 0, h)

        @pl.when(odd)
        def _():
            from_pair(h, -1).start()

        @pl.when(even & (i >= 2))
        def _():
            from_pair(h, 1).start()

    def stage_three(h):
        @pl.when(odd & (i >= 3))
        def _():
            from_pair(h, 1).wait_recv()
            gather(2, 1, h)
            from_two(h).start()

    def send_back(h):
        @pl.when(i >= 3)
        def _():
            from_three(h).start()

        @pl.when(even & (i >= 2) & (h != heads - 2))
        def _():
            from_two(h).start()

        @pl.when(even & (i >= 2) & (h == heads - 1) & (h >= 1))
        def _():
            from_two(heads - 2).start()

    def step(h, c):
        backward_pass(h)
        send_back(h)

        @pl.when(h + 1 < heads)
        def _():
            forward_pass(h + 1)

        stage_two(h - 1)

        @pl.when(h >= 2)
        def _():
            stage_three(h - 2)

        return c

    for h in range(early):
        relay(h)
    for h in range(heads):
        for g in range(GROUPS):
            load_q(h, g).wait()
    for step_ in range(1, chips):
        og_from(step_).wait_recv()
        og_pair(step_, lax.rem(me - 2 * step_ + m, m)).start()
    for step_ in range(1, chips):
        product(lax.rem(me - 2 * step_ + m, m), False)
    forward_pass(0)
    for step_ in range(1, chips):
        s = lax.rem(partner - 2 * step_ + m, m)
        og_pair(step_, s).wait_recv()
        product(s, False)
    for a in range(heads * GROUPS):
        h, g = divmod(a, GROUPS)
        hgt[h, :, g * rows:(g + 1) * rows] = hacc[a * d:(a + 1) * d, :].astype(jnp.bfloat16)
    backward_pass(0)
    send_back(0)
    if heads > 2:
        forward_pass(1)
    for h in range(early, heads):
        relay(h)
    if heads == 2:
        forward_pass(1)
    lax.fori_loop(1, heads, step, 0)
    stage_two(heads - 1)

    def put(h, part):
        dst = dk_ref if part == 0 else dv_ref
        return pltpu.make_async_copy(fin.at[h, part], dst.at[:, pl.ds(h * d, d)], sem_out.at[h, part])

    def finish(h):
        @pl.when(i + 2 < n)
        def _():
            from_two(h).wait_recv()

        @pl.when(even)
        def _():
            from_pair(h, 1).wait_recv()

        total = grad[0, h].astype(jnp.float32)
        total = total + jnp.where(i + 2 < n, back[2, h].astype(jnp.float32), 0.0)
        total = total + jnp.where(even, back[1, h].astype(jnp.float32), 0.0)
        fin[h] = total.astype(jnp.bfloat16)
        for part in range(2):
            put(h, part).start()

    if heads >= 2:
        stage_three(heads - 2)
    stage_three(heads - 1)


    for h in range(heads):
        finish(h)

    for h in range(heads):
        for g in range(GROUPS):
            put_dq(h, g).wait()
        for part in range(2):
            put(h, part).wait()

        @pl.when(i + 2 < n)
        def _():
            two(h).wait_send()

        @pl.when(even | (i >= 3))
        def _():
            pair_even(h).wait_send()

        @pl.when((i >= 1) & (i + 2 < n))
        def _():
            three(h).wait_send()

        @pl.when(i >= 3)
        def _():
            from_three(h).wait_send()

        @pl.when(odd | (i >= 2))
        def _():
            from_pair(h, 1).wait_send()

        @pl.when(i >= 2)
        def _():
            from_two(h).wait_send()

    for hop in range(1, SPAN):

        @pl.when(i + hop < n)
        def _():
            send_ids(hop).wait_send()

    for stp in range(1, chips):
        og_across(stp).wait_send()
    for stp in range(chips):
        og_pair(stp, me).wait_send()


def put_out(a_ref, b_ref, c_ref, x_ref, y_ref, z_ref):
    x_ref[...] = a_ref[...]
    y_ref[...] = b_ref[...]
    z_ref[...] = c_ref[...]


def body(n, m, queries, keys, values, out_grad, doc_ids, w_out):
    rows = queries.shape[0]
    heads = keys.shape[1] // HEAD_SIZE
    width = out_grad.shape[1]
    d = HEAD_SIZE
    wide = GROUPS * rows
    chips = m // 2
    any_space = pl.BlockSpec(memory_space=pl.ANY)
    bf, f32 = jnp.bfloat16, jnp.float32
    dma = pltpu.SemaphoreType.DMA
    w_rows = w_out.shape[0]
    if width % 128:
        w_out = jnp.transpose(w_out.reshape(w_rows, m, width), (1, 0, 2))
    results = pl.pallas_call(
        functools.partial(kernel, n, m, heads, rows, width),
        out_shape=(
            jax.ShapeDtypeStruct(queries.shape, bf),
            jax.ShapeDtypeStruct(keys.shape, bf),
            jax.ShapeDtypeStruct(values.shape, bf),
        ),
        in_specs=[pl.BlockSpec(memory_space=pltpu.VMEM)] + [any_space] * 5,
        out_specs=(any_space,) * 3,
        scratch_shapes=[
            pltpu.VMEM((SPAN, heads, 2, rows, d), bf),
            pltpu.VMEM((m, rows, width), bf),
            pltpu.VMEM((m, w_rows, width), bf),
            pltpu.VMEM((heads, wide, d), bf),
            pltpu.VMEM((heads * GROUPS * d, rows), f32),
            pltpu.VMEM((heads, d, wide), bf),
            [pltpu.VMEM((rows,), jnp.int32)] * (SPAN - 1),
            pltpu.VMEM((SPAN, rows, wide), f32),
            pltpu.VMEM((SPAN, rows, wide), f32),
            pltpu.VMEM((SPAN, rows, wide), bf),
            pltpu.VMEM((d, wide), f32),
            pltpu.VMEM((1, wide), f32),
            pltpu.VMEM((SPAN, heads, 2, rows, d), bf),
            pltpu.VMEM((3, heads, 2, rows, d), bf),
            pltpu.VMEM((heads, wide, d), bf),
            pltpu.VMEM((heads, 2, rows, d), bf),
            dma((heads, 2)),
            dma((heads, GROUPS)),
            dma,
            dma((m,)),
            dma((heads, 2)),
            dma((SPAN - 1,)),
            dma((SPAN - 1,)),
            dma((3, heads)),
            dma((3, heads)),
            dma((3, heads)),
            dma((3, heads)),
            dma((2 * chips - 1,)),
            dma((2 * chips - 1,)),
        ],
        compiler_params=pltpu.CompilerParams(
            collective_id=0, has_side_effects=True, vmem_limit_bytes=60 * 1024 * 1024
        ),
    )(doc_ids, queries, keys, values, out_grad, w_out)

    blocks = 2
    specs = [pl.BlockSpec((rows // blocks, r.shape[1]), lambda b: (b, 0)) for r in results]
    return pl.pallas_call(
        put_out,
        grid=(blocks,),
        out_shape=tuple(jax.ShapeDtypeStruct(r.shape, bf) for r in results),
        in_specs=specs,
        out_specs=tuple(specs),
    )(*results)


def solution(mesh):
    placed = (
        P("ctx", "mp"),
        P("ctx", "mp"),
        P("ctx", "mp"),
        P("ctx", "mp"),
        P("ctx"),
        P("mp", None),
    )
    return jax.shard_map(
        functools.partial(body, mesh.shape["ctx"], mesh.shape["mp"]),
        mesh=mesh,
        in_specs=placed,
        out_specs=(P("ctx", "mp"), P("ctx", "mp"), P("ctx", "mp")),
        check_vma=False,
    )
```
